32 devices in a mesh: peer: 8 (over y, x, core), zero: 4 (over z).
Axes of the slice: x: 2, y: 2, z: 4, core: 2. Of those that a mesh axis runs over, the one named last changes fastest.
Arguments:
- tokens: bfloat16 [8, 2048, 1024], P('peer', 'zero'), may hold values from -6 to 6
- out_grad: bfloat16 [8, 2048, 1024], P('peer', 'zero'), may hold values from -6 to 6
- step: int32 [1], replicated, may hold values from 0 to 3999
- up_param: float32 [8, 1024, 2048], P('peer', 'zero'), may hold values from -0.2 to 0.2
- down_param: float32 [8, 2048, 1024], P('peer', 'zero'), may hold values from -0.2 to 0.2
- up_first: float32 [8, 1024, 2048], P('peer', 'zero'), may hold values from -27.1529 to 27.1529
- down_first: float32 [8, 2048, 1024], P('peer', 'zero'), may hold values from -27.1529 to 27.1529
- up_second: float32 [8, 1024, 2048], P('peer', 'zero'), may hold values from 0.8192 to 819.2
- down_second: float32 [8, 2048, 1024], P('peer', 'zero'), may hold values from 0.8192 to 819.2
Outputs:
- new_up: float32 [8, 1024, 2048], P('peer', 'zero')
- new_down: float32 [8, 2048, 1024], P('peer', 'zero')
- new_up_first: float32 [8, 1024, 2048], P('peer', 'zero')
- new_down_first: float32 [8, 2048, 1024], P('peer', 'zero')
- new_up_second: float32 [8, 1024, 2048], P('peer', 'zero')
- new_down_second: float32 [8, 2048, 1024], P('peer', 'zero')
The draws below stay inside these ranges and needn't reach their ends.
All inputs are finite; a program needn't handle non-finite values.
Results may differ from the reference program's by a relative error of at most 0.0065.
Values may be sent and summed in bfloat16 or wider, within the bound.
A program may use at most 128 MiB of HBM per device.

```python
import math
import jax
import jax.numpy as jnp
from jax import lax

D = 1024
FFW = 2048
GTOK = 2048
GROUPS = 8
N_PEER = 8


def block_levels(key, shape, cuts, low, high):
    level = 1.0
    for position, blocks in cuts:
        steps = jax.random.uniform(jax.random.fold_in(jax.random.fold_in(key, 6), position), (blocks,), jnp.float32, low / len(cuts), high / len(cuts))
        level = level * jnp.repeat(jnp.exp(steps), shape[position] // blocks).reshape((-1,) + (1,) * (len(shape) - 1 - position))
    return level


def scatter_about(own_key, shape, width, limit, pieces=(), held_as=jnp.bfloat16):
    values = width * jax.random.normal(own_key, shape, jnp.float32)
    if pieces:
        values = values * block_levels(own_key, shape, pieces, -0.22, 0.18)
    return jnp.clip(values, -limit, limit).astype(held_as)


def setup_inputs(seed: int = 0) -> dict:
    splits = jax.random.split(jax.random.key(seed), 10)
    tokens = scatter_about(splits[0], (GROUPS, GTOK, D), 1.0, 6.0, ((0, 8), (1, 4)))
    out_grad = scatter_about(splits[1], (GROUPS, GTOK, D), 1.0, 6.0, ((0, 8), (1, 4)))
    step = jax.random.randint(splits[2], (1,), 0, 4000).astype(jnp.int32)
    up_param = scatter_about(splits[3], (GROUPS, D, FFW), 0.03, 0.2, ((0, 8), (1, 4)), jnp.float32)
    down_param = scatter_about(splits[4], (GROUPS, FFW, D), 0.03, 0.2, ((0, 8), (1, 4)), jnp.float32)
    up_first = scatter_about(splits[5], (GROUPS, D, FFW), (0.1 * GTOK ** 0.5), 27.1529, ((0, 8), (1, 4)), jnp.float32)
    down_first = scatter_about(splits[6], (GROUPS, FFW, D), (0.1 * GTOK ** 0.5), 27.1529, ((0, 8), (1, 4)), jnp.float32)
    up_second = jnp.clip(jnp.exp(math.log(819.2) - 6.9077553 * jax.random.uniform(splits[7], (GROUPS, D, FFW), jnp.float32) ** block_levels(splits[7], (GROUPS, D, FFW), ((0, 8), (1, 4)), -0.2, 0.2)), 0.8192, 819.2)
    down_second = jnp.clip(jnp.exp(math.log(819.2) - 6.9077553 * jax.random.uniform(splits[8], (GROUPS, FFW, D), jnp.float32) ** block_levels(splits[8], (GROUPS, FFW, D), ((0, 8), (1, 4)), -0.2, 0.2)), 0.8192, 819.2)
    return {"tokens": tokens, "out_grad": out_grad, "step": step, "up_param": up_param, "down_param": down_param, "up_first": up_first, "down_first": down_first, "up_second": up_second, "down_second": down_second}


def gelu_tanh(values):
    return 0.5 * values * (1.0 + jnp.tanh(0.7978845608 * (values + 0.044715 * values * values * values)))

def group_grads(items):
    tokens, out_grad, up_param, down_param = items
    widened = tokens.astype(jnp.float32)
    center = lax.optimization_barrier(jnp.mean(widened, axis=1, keepdims=True))
    spread = lax.optimization_barrier(jnp.mean((widened - center) * (widened - center), axis=1, keepdims=True))
    normed = ((widened - center) * lax.rsqrt(spread + 1e-05)).astype(jnp.bfloat16)
    up_low = up_param.astype(jnp.bfloat16)
    down_low = down_param.astype(jnp.bfloat16)
    pre = jnp.dot(normed, up_low, preferred_element_type=jnp.float32)
    active, backward = jax.vjp(gelu_tanh, pre)
    act = active.astype(jnp.bfloat16)
    act_grad = jnp.dot(out_grad, down_low.T, preferred_element_type=jnp.float32)
    pre_grad = backward(act_grad)[0].astype(jnp.bfloat16)
    up_grad = jnp.dot(normed.T, pre_grad, preferred_element_type=jnp.float32)
    down_grad = jnp.dot(act.T, out_grad, preferred_element_type=jnp.float32)
    return (up_grad, down_grad)

def adam_update(param, first, second, grad, first_fix, second_fix):
    first_new = 0.9 * first + 0.1 * grad
    second_new = 0.999 * second + 0.001 * grad * grad
    local = param - 0.01 * (first_new / first_fix) / (jnp.sqrt(second_new / second_fix) + 1e-08)
    return (local, first_new, second_new)

def reference(tokens, out_grad, step, up_param, down_param, up_first, down_first, up_second, down_second):
    up_grad, down_grad = lax.map(group_grads, (tokens, out_grad, up_param, down_param))
    count = (step[0] + 1).astype(jnp.float32)
    first_fix = 1.0 - jnp.power(jnp.float32(0.9), count)
    second_fix = 1.0 - jnp.power(jnp.float32(0.999), count)
    up_local, up_first_new, up_second_new = adam_update(up_param, up_first, up_second, up_grad, first_fix, second_fix)
    down_local, down_first_new, down_second_new = adam_update(down_param, down_first, down_second, down_grad, first_fix, second_fix)
    levels = N_PEER.bit_length() - 1
    distance = jnp.left_shift(jnp.int32(1), (step[0] % levels).astype(jnp.int32))
    partner = ((jnp.arange(N_PEER, dtype=jnp.int32) + distance) % N_PEER).astype(jnp.int32)
    new_up = 0.5 * (up_local + jnp.take(up_local, partner, axis=0))
    new_down = 0.5 * (down_local + jnp.take(down_local, partner, axis=0))
    return (new_up, new_down, up_first_new, down_first_new, up_second_new, down_second_new)
```

```python
from functools import partial

import jax
import jax.numpy as jnp
from jax import lax
from jax.experimental import pallas as pl
from jax.experimental.pallas import tpu as pltpu
from jax.sharding import PartitionSpec as P

MIB = 2**20
BF16, F32 = jnp.bfloat16, jnp.float32
EARLY = 1


def step_kernel(
    dist,
    dims,
    fixes,
    tok_in,
    out_in,
    up_in,
    down_in,
    up_first_in,
    down_first_in,
    up_second_in,
    down_second_in,
    up,
    down,
    up_first,
    down_first,
    up_second,
    down_second,
    toks,
    outs,
    normed,
    normed_t,
    up_stage,
    down_stage,
    up_cols,
    down_rows,
    act_t,
    pre_grad,
    up_grad,
    down_grad,
    up_got,
    down_got,
    up_mine,
    down_mine,
    up_other,
    down_other,
    load_sem,
    tok_send,
    tok_recv,
    fwd_send,
    upw_send,
    upw_recv,
    downw_send,
    downw_recv,
    upg_send,
    upg_recv,
    downg_send,
    downg_recv,
    upl_send,
    upl_recv,
    downl_send,
    downl_recv,
):
    n, tokens, width, units, unit_block, chunk = dims
    half = n // 2
    rows = width // n
    owned = units // n
    per_owner = owned // unit_block
    steps = per_owner * half
    chunks = tokens // chunk
    total = n * tokens

    z, p = lax.axis_index("zero"), lax.axis_index("peer")
    peers = lax.axis_size("peer")
    side = lax.rem(p, 2)
    base = p - side
    center = half - 1 + side
    worker = (z == half - 1) | (z == half)
    first = worker & (z == center)
    group = base + z - (half - 1)
    z_slot = lax.rem(z, half)
    z_half = lax.div(z, half)

    def at(peer, zero):
        return {"peer": peer, "zero": zero}

    def remote(src, dst, send, recv, peer, zero):
        return pltpu.make_async_remote_copy(
            src_ref=src,
            dst_ref=dst,
            send_sem=send,
            recv_sem=recv,
            device_id=at(peer, zero),
            device_id_type=pl.DeviceIdType.MESH,
        )

    def landed(dst, sem):
        pltpu.make_async_copy(dst, dst, sem).wait()

    def block_of(which, step):
        return which * steps + lax.rem(step, half) * per_owner + lax.div(step, half)

    def span(start, size):
        return pl.ds(pl.multiple_of(start * size, size), size)

    params = [pltpu.make_async_copy(up_in, up, load_sem.at[0])]
    params.append(pltpu.make_async_copy(down_in, down, load_sem.at[1]))
    states = [
        pltpu.make_async_copy(src, dst, load_sem.at[2 + index])
        for index, (src, dst) in enumerate(
            (
                (up_first_in, up_first),
                (down_first_in, down_first),
                (up_second_in, up_second),
                (down_second_in, down_second),
            )
        )
    ]
    for copy in params:
        copy.start()

    barrier = pltpu.get_barrier_semaphore()

    def greet(peer, zero):
        pl.semaphore_signal(
            barrier, inc=1, device_id=at(peer, zero), device_id_type=pl.DeviceIdType.MESH
        )

    for hop in range(1, n):
        for other in range(2):
            greet(base + other, lax.rem(z + hop, n))
    greet(base + 1 - side, z)
    ahead, behind = lax.rem(p + dist, peers), lax.rem(p + peers - dist, peers)
    greet(ahead, z)
    greet(behind, z)
    pl.semaphore_wait(barrier, 2 * n + 1)

    sources, held = (tok_in, out_in), (toks, outs)

    def place(owner, piece):
        return span(owner * chunks + piece, chunk)

    def give(which, piece):
        return remote(
            sources[which].at[span(piece, chunk)],
            held[which].at[place(z, piece)],
            tok_send.at[which, piece],
            tok_recv.at[which, z, piece],
            jnp.where(z == center, base + 1 - side, p),
            center,
        )

    def keep(which, piece):
        return pltpu.make_async_copy(
            sources[which].at[span(piece, chunk)],
            held[which].at[place(z, piece)],
            tok_recv.at[which, z, piece],
        )

    def forward(which, owner, piece):
        spot = held[which].at[place(owner, piece)]
        return remote(
            spot,
            spot,
            fwd_send.at[which, owner, piece],
            tok_recv.at[which, owner, piece],
            base + 1 - side,
            z,
        )

    for piece in range(chunks):
        for which in range(2):
            give(which, piece).start()

            @pl.when(first)
            def _():
                keep(which, piece).start()

    for copy in params:
        copy.wait()
    for copy in states:
        copy.start()

    def give_up(which, step):
        index = which * steps + step
        src, dst = up_stage.at[index], up_cols.at[step, span(z, rows)]
        own = partial(pltpu.make_async_copy, src, dst, upw_recv.at[step, z])
        sent = partial(
            remote, src, dst, upw_send.at[which, step], upw_recv.at[step, z], base + which, center
        )
        return own, sent, (z == center) & (side == which)

    def give_down(piece):
        step = piece * half + z_slot
        src, dst = down_stage.at[piece], down_rows.at[step]
        own = partial(pltpu.make_async_copy, src, dst, downw_recv.at[step])
        sent = partial(
            remote, src, dst, downw_send.at[piece], downw_recv.at[step], base + z_half, center
        )
        return own, sent, (z == center) & (side == z_half)

    def begin(copies):
        own, sent, mine = copies

        @pl.when(mine)
        def _():
            own().start()

        @pl.when(jnp.logical_not(mine))
        def _():
            sent().start()

    def finish_send(copies):
        _, sent, mine = copies

        @pl.when(jnp.logical_not(mine))
        def _():
            sent().wait_send()

    for step in range(steps):
        for which in range(2):
            block = which * steps + (step % half) * per_owner + step // half
            up_stage[which * steps + step] = up[
                :, block * unit_block : (block + 1) * unit_block
            ].astype(BF16)
            begin(give_up(which, step))
        if step % half == 0:
            piece = step // half
            down_stage[piece] = down[piece * unit_block : (piece + 1) * unit_block].astype(BF16)

        @pl.when(z_slot == step % half)
        def _():
            begin(give_down(step // half))

    @pl.when(worker)
    def _():
        @pl.loop(0, chunks)
        def _(piece):
            @pl.loop(0, n)
            def _(owner):
                spot = place(owner, piece)
                for which in range(2):
                    landed(held[which].at[spot], tok_recv.at[which, owner, piece])

                    @pl.when(first & (owner != z))
                    def _():
                        forward(which, owner, piece).start()

                wide = toks[spot, :].astype(F32)
                mean = jnp.mean(wide, axis=1, keepdims=True)
                wide = wide - mean
                spread = jnp.mean(wide * wide, axis=1, keepdims=True)
                wide = wide * lax.rsqrt(spread + 1e-05)
                normed[spot, :] = wide.astype(BF16)
                normed_t[:, spot] = wide.T.astype(BF16)

    tile = min(total, 256)

    def give_grads(step, owner):
        src, dst = up_grad.at[step, span(owner, rows)], up_got.at[side * steps + step]
        own = partial(pltpu.make_async_copy, src, dst, upg_recv.at[side, step])
        sent = partial(
            remote, src, dst, upg_send.at[step, owner], upg_recv.at[side, step], group, owner
        )
        return own, sent, first & (owner == z)

    def give_down_grads(step):
        owner = side * half + lax.rem(step, half)
        piece = lax.div(step, half)
        src, dst = down_grad.at[step], down_got.at[piece]
        own = partial(pltpu.make_async_copy, src, dst, downg_recv.at[piece])
        sent = partial(
            remote, src, dst, downg_send.at[step], downg_recv.at[piece], group, owner
        )
        return own, sent, first & (owner == z)

    def spread_grads(step, far):
        for slot in range(half):
            owner = jnp.where((z_half == 0) != far, slot, half + slot)
            begin(give_grads(step, owner))

        @pl.when((side == z_half) != far)
        def _():
            begin(give_down_grads(step))

    def compute(step):
        for owner in range(n):
            landed(up_cols.at[step, pl.ds(owner * rows, rows)], upw_recv.at[step, owner])
        landed(down_rows.at[step], downw_recv.at[step])

        @pl.when(step == steps - 1)
        def _():
            @pl.loop(EARLY, steps - 1)
            def _(late):
                spread_grads(late, True)

        @pl.loop(0, total // tile)
        def _(index):
            part = span(index, tile)
            pre = jnp.dot(normed[part, :], up_cols[step], preferred_element_type=F32)
            act_grad = lax.dot_general(
                outs[part, :], down_rows[step], (((1,), (1,)), ((), ())), preferred_element_type=F32
            )
            square = pre * pre
            bend = jnp.tanh(pre * (0.7978845608 + (0.7978845608 * 0.044715) * square))
            lift = 0.5 + 0.5 * bend
            slope = lift + (0.5 * pre) * (1.0 - bend * bend) * (
                0.7978845608 + (3.0 * 0.7978845608 * 0.044715) * square
            )
            act_t[:, part] = (pre * lift).T.astype(BF16)
            pre_grad[part, :] = (act_grad * slope).astype(BF16)

        @pl.loop(0, width // unit_block)
        def _(index):
            part = span(index, unit_block)
            down_grad[step, :, part] = jnp.dot(
                act_t[...], outs[:, part], preferred_element_type=F32
            ).astype(BF16)
            up_grad[step, part, :] = jnp.dot(
                normed_t[part, :], pre_grad[...], preferred_element_type=F32
            ).astype(BF16)

        spread_grads(step, False)

        @pl.when((step < EARLY) | (step == steps - 1))
        def _():
            spread_grads(step, True)

    first_scale, second_scale = fixes[0], fixes[1]

    def adam(param, first_ref, second_ref, got, mine, window, piece_window):
        grad = got[piece_window].astype(F32)
        first_new = 0.9 * first_ref[window] + 0.1 * grad
        second_new = 0.999 * second_ref[window] + 0.001 * grad * grad
        first_ref[window] = first_new
        second_ref[window] = second_new
        local = param[window] - (first_new * first_scale) / (
            jnp.sqrt(second_new * second_scale) + 1e-08
        )
        param[window] = local
        mine[piece_window] = local.astype(BF16)

    up_tile, down_tile = min(rows, 32), min(unit_block, 16)

    def pass_up(which, step):
        index = which * steps + step
        return remote(
            up_mine.at[index],
            up_other.at[index],
            upl_send.at[which, step],
            upl_recv.at[which, step],
            behind,
            z,
        )

    def pass_down(piece):
        return remote(
            down_mine.at[piece],
            down_other.at[piece],
            downl_send.at[piece],
            downl_recv.at[piece],
            behind,
            z,
        )

    def update(step):
        for which in range(2):
            index = which * steps + step
            columns = span(block_of(which, step), unit_block)
            landed(up_got.at[index], upg_recv.at[which, step])

            @pl.loop(0, rows // up_tile)
            def _(part):
                some = span(part, up_tile)
                adam(
                    up, up_first, up_second, up_got, up_mine, (some, columns), (index, some)
                )

            pass_up(which, step).start()

        @pl.when(lax.rem(step, half) == z_slot)
        def _():
            piece = lax.div(step, half)
            landed(down_got.at[piece], downg_recv.at[piece])

            @pl.loop(0, unit_block // down_tile)
            def _(part):
                some = span(part, down_tile)
                window = span(piece * (unit_block // down_tile) + part, down_tile)
                adam(
                    down, down_first, down_second, down_got, down_mine, (window,), (piece, some)
                )

            pass_down(piece).start()

    def average(step):
        for which in range(2):
            index = which * steps + step
            columns = span(block_of(which, step), unit_block)
            landed(up_other.at[index], upl_recv.at[which, step])
            up[:, columns] = 0.5 * (up[:, columns] + up_other[index].astype(F32))

        @pl.when(lax.rem(step, half) == z_slot)
        def _():
            piece = lax.div(step, half)
            landed(down_other.at[piece], downl_recv.at[piece])
            window = span(piece, unit_block)
            down[window, :] = 0.5 * (down[window, :] + down_other[piece].astype(F32))

    for copy in states:
        copy.wait()
    delay = jnp.where(worker, jnp.where(first, 1, steps), 0)

    @pl.loop(0, 2 * steps)
    def _(turn):
        @pl.when(worker & (turn < steps))
        def _():
            compute(turn)

        @pl.when((turn >= delay) & (turn < delay + steps))
        def _():
            update(turn - delay)

    @pl.loop(0, steps)
    def _(step):
        average(step)

    for piece in range(chunks):
        for which in range(2):
            give(which, piece).wait_send()

    @pl.when(first)
    def _():
        @pl.loop(0, chunks)
        def _(piece):
            for which in range(2):

                @pl.loop(0, n)
                def _(owner):
                    @pl.when(owner != z)
                    def _():
                        forward(which, owner, piece).wait_send()

    @pl.loop(0, steps)
    def _(step):
        for which in range(2):
            finish_send(give_up(which, step))
            pass_up(which, step).wait_send()

        @pl.when(z_slot == lax.rem(step, half))
        def _():
            finish_send(give_down(lax.div(step, half)))
            pass_down(lax.div(step, half)).wait_send()

        @pl.when(worker)
        def _():
            for owner in range(n):
                finish_send(give_grads(step, owner))
            finish_send(give_down_grads(step))


def fused_step(dist, name, fixes, tokens, out_grad, params):
    n = lax.axis_size("zero")
    own_tokens, width = tokens.shape
    owned = params[1].shape[0]
    units = owned * n
    rows = width // n
    block = min(owned, 256)
    steps = (owned // block) * (n // 2)
    pieces = owned // block
    chunk = min(own_tokens, 128)
    chunks = own_tokens // chunk
    total = n * own_tokens
    dims = (n, own_tokens, width, units, block, chunk)
    hbm = pl.BlockSpec(memory_space=pltpu.HBM)
    vmem = pl.BlockSpec(memory_space=pltpu.VMEM)
    dma = pltpu.SemaphoreType.DMA
    up_shape = jax.ShapeDtypeStruct((rows, units), F32)
    down_shape = jax.ShapeDtypeStruct((owned, width), F32)
    return pl.pallas_call(
        partial(step_kernel, dist, dims),
        out_shape=(up_shape, down_shape) * 3,
        in_specs=[pl.BlockSpec(memory_space=pltpu.SMEM)] + [hbm] * 8,
        out_specs=(vmem,) * 6,
        scratch_shapes=[
            pltpu.VMEM((total, width), BF16),
            pltpu.VMEM((total, width), BF16),
            pltpu.VMEM((total, width), BF16),
            pltpu.VMEM((width, total), BF16),
            pltpu.VMEM((2 * steps, rows, block), BF16),
            pltpu.VMEM((pieces, block, width), BF16),
            pltpu.VMEM((steps, width, block), BF16),
            pltpu.VMEM((steps, block, width), BF16),
            pltpu.VMEM((block, total), BF16),
            pltpu.VMEM((total, block), BF16),
            pltpu.VMEM((steps, width, block), BF16),
            pltpu.VMEM((steps, block, width), BF16),
            pltpu.VMEM((2 * steps, rows, block), BF16),
            pltpu.VMEM((pieces, block, width), BF16),
            pltpu.VMEM((2 * steps, rows, block), BF16),
            pltpu.VMEM((pieces, block, width), BF16),
            pltpu.VMEM((2 * steps, rows, block), BF16),
            pltpu.VMEM((pieces, block, width), BF16),
            dma((6,)),
            dma((2, chunks)),
            dma((2, n, chunks)),
            dma((2, n, chunks)),
            dma((2, steps)),
            dma((steps, n)),
            dma((pieces,)),
            dma((steps,)),
            dma((steps, n)),
            dma((2, steps)),
            dma((steps,)),
            dma((pieces,)),
            dma((2, steps)),
            dma((2, steps)),
            dma((pieces,)),
            dma((pieces,)),
        ],
        compiler_params=pltpu.CompilerParams(
            collective_id=name, has_side_effects=True, vmem_limit_bytes=46 * MIB
        ),
    )(fixes, tokens, out_grad, *params)


def body(
    tokens, out_grad, step, up_param, down_param, up_first, down_first, up_second, down_second
):
    count = (step[0] + 1).astype(F32)
    first_fix = 1.0 - jnp.power(F32(0.9), count)
    second_fix = 1.0 - jnp.power(F32(0.999), count)
    fixes = jnp.stack([0.01 / first_fix, 1.0 / second_fix])
    params = (up_param, down_param, up_first, down_first, up_second, down_second)
    operands = (fixes, tokens[0], out_grad[0], tuple(array[0] for array in params))
    levels = lax.axis_size("peer").bit_length() - 1
    branches = [
        lambda args, level=level: fused_step(2**level, level, *args) for level in range(levels)
    ]
    results = lax.switch(step[0] % levels, branches, operands)
    return tuple(array[None] for array in results)


def solution(mesh):
    spec = P("peer", "zero", None)
    return jax.shard_map(
        body,
        mesh=mesh,
        in_specs=(spec, spec, P()) + (spec,) * 6,
        out_specs=(spec,) * 6,
        check_vma=False,
    )
```

```python
from functools import partial

import jax
import jax.numpy as jnp
from jax import lax
from jax.experimental import pallas as pl
from jax.experimental.pallas import tpu as pltpu
from jax.sharding import PartitionSpec as P

MIB = 2**20
BF16, F32 = jnp.bfloat16, jnp.float32
EARLY = 1
STRIP = 64


def step_kernel(
    dist,
    dims,
    fixes,
    tok_in,
    out_in,
    up_in,
    down_in,
    up_first_in,
    down_first_in,
    up_second_in,
    down_second_in,
    up,
    down,
    up_first,
    down_first,
    up_second,
    down_second,
    toks,
    outs,
    normed,
    normed_t,
    up_stage,
    down_stage,
    up_cols,
    down_rows,
    act_t,
    pre_grad,
    up_grad,
    down_grad,
    up_got,
    down_got,
    up_mine,
    down_mine,
    up_other,
    down_other,
    load_sem,
    tok_send,
    tok_recv,
    fwd_send,
    upw_send,
    upw_recv,
    downw_send,
    downw_recv,
    upg_send,
    upg_recv,
    downg_send,
    downg_recv,
    upl_send,
    upl_recv,
    downl_send,
    downl_recv,
):
    n, tokens, width, units, unit_block, chunk, strip = dims
    half = n // 2
    rows = width // n
    owned = units // n
    per_owner = owned // unit_block
    steps = per_owner * half
    chunks = tokens // chunk
    strips = unit_block // strip
    total = n * tokens

    z, p = lax.axis_index("zero"), lax.axis_index("peer")
    peers = lax.axis_size("peer")
    side = lax.rem(p, 2)
    base = p - side
    center = half - 1 + side
    worker = (z == half - 1) | (z == half)
    first = worker & (z == center)
    group = base + z - (half - 1)
    z_slot = lax.rem(z, half)
    z_half = lax.div(z, half)

    def at(peer, zero):
        return {"peer": peer, "zero": zero}

    def remote(src, dst, send, recv, peer, zero):
        return pltpu.make_async_remote_copy(
            src_ref=src,
            dst_ref=dst,
            send_sem=send,
            recv_sem=recv,
            device_id=at(peer, zero),
            device_id_type=pl.DeviceIdType.MESH,
        )

    def landed(dst, sem):
        pltpu.make_async_copy(dst, dst, sem).wait()

    def block_of(which, step):
        return which * steps + lax.rem(step, half) * per_owner + lax.div(step, half)

    def span(start, size):
        return pl.ds(pl.multiple_of(start * size, size), size)

    params = [pltpu.make_async_copy(up_in, up, load_sem.at[0])]
    params.append(pltpu.make_async_copy(down_in, down, load_sem.at[1]))
    states = [
        pltpu.make_async_copy(src, dst, load_sem.at[2 + index])
        for index, (src, dst) in enumerate(
            (
                (up_first_in, up_first),
                (down_first_in, down_first),
                (up_second_in, up_second),
                (down_second_in, down_second),
            )
        )
    ]
    for copy in params:
        copy.start()

    barrier = pltpu.get_barrier_semaphore()

    def greet(peer, zero):
        pl.semaphore_signal(
            barrier, inc=1, device_id=at(peer, zero), device_id_type=pl.DeviceIdType.MESH
        )

    for hop in range(1, n):
        for other in range(2):
            greet(base + other, lax.rem(z + hop, n))
    greet(base + 1 - side, z)
    ahead, behind = lax.rem(p + dist, peers), lax.rem(p + peers - dist, peers)
    greet(ahead, z)
    greet(behind, z)
    pl.semaphore_wait(barrier, 2 * n + 1)

    sources, held = (tok_in, out_in), (toks, outs)

    def place(owner, piece):
        return span(owner * chunks + piece, chunk)

    def give(which, piece):
        return remote(
            sources[which].at[span(piece, chunk)],
            held[which].at[place(z, piece)],
            tok_send.at[which, piece],
            tok_recv.at[which, z, piece],
            jnp.where(z == center, base + 1 - side, p),
            center,
        )

    def keep(which, piece):
        return pltpu.make_async_copy(
            sources[which].at[span(piece, chunk)],
            held[which].at[place(z, piece)],
            tok_recv.at[which, z, piece],
        )

    def forward(which, owner, piece):
        spot = held[which].at[place(owner, piece)]
        return remote(
            spot,
            spot,
            fwd_send.at[which, owner, piece],
            tok_recv.at[which, owner, piece],
            base + 1 - side,
            z,
        )

    for piece in range(chunks):
        for which in range(2):
            give(which, piece).start()

            @pl.when(first)
            def _():
                keep(which, piece).start()

    for copy in params:
        copy.wait()
    for copy in states:
        copy.start()

    def give_up(which, step):
        index = which * steps + step
        src, dst = up_stage.at[index], up_cols.at[step, span(z, rows)]
        own = partial(pltpu.make_async_copy, src, dst, upw_recv.at[step, z])
        sent = partial(
            remote, src, dst, upw_send.at[which, step], upw_recv.at[step, z], base + which, center
        )
        return own, sent, (z == center) & (side == which)

    def give_down(piece):
        step = piece * half + z_slot
        src, dst = down_stage.at[piece], down_rows.at[step]
        own = partial(pltpu.make_async_copy, src, dst, downw_recv.at[step])
        sent = partial(
            remote, src, dst, downw_send.at[piece], downw_recv.at[step], base + z_half, center
        )
        return own, sent, (z == center) & (side == z_half)

    def begin(copies):
        own, sent, mine = copies

        @pl.when(mine)
        def _():
            own().start()

        @pl.when(jnp.logical_not(mine))
        def _():
            sent().start()

    def finish_send(copies):
        _, sent, mine = copies

        @pl.when(jnp.logical_not(mine))
        def _():
            sent().wait_send()

    for step in range(steps):
        for which in range(2):
            block = which * steps + (step % half) * per_owner + step // half
            up_stage[which * steps + step] = up[
                :, block * unit_block : (block + 1) * unit_block
            ].astype(BF16)
            begin(give_up(which, step))
        if step % half == 0:
            piece = step // half
            down_stage[piece] = down[piece * unit_block : (piece + 1) * unit_block].astype(BF16)

        @pl.when(z_slot == step % half)
        def _():
            begin(give_down(step // half))

    @pl.when(worker)
    def _():
        @pl.loop(0, chunks)
        def _(piece):
            @pl.loop(0, n)
            def _(owner):
                spot = place(owner, piece)
                for which in range(2):
                    landed(held[which].at[spot], tok_recv.at[which, owner, piece])

                    @pl.when(first & (owner != z))
                    def _():
                        forward(which, owner, piece).start()

                wide = toks[spot, :].astype(F32)
                mean = jnp.mean(wide, axis=1, keepdims=True)
                wide = wide - mean
                spread = jnp.mean(wide * wide, axis=1, keepdims=True)
                wide = wide * lax.rsqrt(spread + 1e-05)
                normed[spot, :] = wide.astype(BF16)
                normed_t[:, spot] = wide.T.astype(BF16)

    tile = min(total, 256)

    def give_grads(step, owner):
        src, dst = up_grad.at[step, span(owner, rows)], up_got.at[side * steps + step]
        own = partial(pltpu.make_async_copy, src, dst, upg_recv.at[side, step])
        sent = partial(
            remote, src, dst, upg_send.at[step, owner], upg_recv.at[side, step], group, owner
        )
        return own, sent, first & (owner == z)

    def give_down_grads(step, part):
        owner = side * half + lax.rem(step, half)
        piece = lax.div(step, half)
        some = span(part, strip)
        src, dst = down_grad.at[step, some], down_got.at[piece, some]
        own = partial(pltpu.make_async_copy, src, dst, downg_recv.at[piece, part])
        sent = partial(
            remote, src, dst, downg_send.at[step, part], downg_recv.at[piece, part], group, owner
        )
        return own, sent, first & (owner == z)

    def spread_grads(step, far):
        for slot in range(half):
            owner = jnp.where((z_half == 0) != far, slot, half + slot)
            begin(give_grads(step, owner))

        @pl.when((side == z_half) != far)
        def _():
            @pl.loop(0, strips)
            def _(part):
                begin(give_down_grads(step, part))

    def compute(step):
        for owner in range(n):
            landed(up_cols.at[step, pl.ds(owner * rows, rows)], upw_recv.at[step, owner])
        landed(down_rows.at[step], downw_recv.at[step])

        @pl.when(step == steps - 1)
        def _():
            @pl.loop(EARLY, steps - 1)
            def _(late):
                spread_grads(late, True)

        @pl.loop(0, total // tile)
        def _(index):
            part = span(index, tile)
            pre = jnp.dot(normed[part, :], up_cols[step], preferred_element_type=F32)
            act_grad = lax.dot_general(
                outs[part, :], down_rows[step], (((1,), (1,)), ((), ())), preferred_element_type=F32
            )
            square = pre * pre
            bend = jnp.tanh(pre * (0.7978845608 + (0.7978845608 * 0.044715) * square))
            lift = 0.5 + 0.5 * bend
            slope = lift + (0.5 * pre) * (1.0 - bend * bend) * (
                0.7978845608 + (3.0 * 0.7978845608 * 0.044715) * square
            )
            act_t[:, part] = (pre * lift).T.astype(BF16)
            pre_grad[part, :] = (act_grad * slope).astype(BF16)

        @pl.loop(0, width // unit_block)
        def _(index):
            part = span(index, unit_block)
            down_grad[step, :, part] = jnp.dot(
                act_t[...], outs[:, part], preferred_element_type=F32
            ).astype(BF16)
            up_grad[step, part, :] = jnp.dot(
                normed_t[part, :], pre_grad[...], preferred_element_type=F32
            ).astype(BF16)

        spread_grads(step, False)

        @pl.when((step < EARLY) | (step == steps - 1))
        def _():
            spread_grads(step, True)

    first_scale, second_scale = fixes[0], fixes[1]

    def adam(param, first_ref, second_ref, got, mine, window, piece_window):
        grad = got[piece_window].astype(F32)
        first_new = 0.9 * first_ref[window] + 0.1 * grad
        second_new = 0.999 * second_ref[window] + 0.001 * grad * grad
        first_ref[window] = first_new
        second_ref[window] = second_new
        local = param[window] - (first_new * first_scale) / (
            jnp.sqrt(second_new * second_scale) + 1e-08
        )
        param[window] = local
        mine[piece_window] = local.astype(BF16)

    up_tile, down_tile = min(rows, 32), min(strip, 16)

    def pass_up(which, step):
        index = which * steps + step
        return remote(
            up_mine.at[index],
            up_other.at[index],
            upl_send.at[which, step],
            upl_recv.at[which, step],
            behind,
            z,
        )

    def pass_down(piece, part):
        some = span(part, strip)
        return remote(
            down_mine.at[piece, some],
            down_other.at[piece, some],
            downl_send.at[piece, part],
            downl_recv.at[piece, part],
            behind,
            z,
        )

    def update(step):
        for which in range(2):
            index = which * steps + step
            columns = span(block_of(which, step), unit_block)
            landed(up_got.at[index], upg_recv.at[which, step])

            @pl.loop(0, rows // up_tile)
            def _(part):
                some = span(part, up_tile)
                adam(
                    up, up_first, up_second, up_got, up_mine, (some, columns), (index, some)
                )

            pass_up(which, step).start()

        @pl.when(lax.rem(step, half) == z_slot)
        def _():
            piece = lax.div(step, half)

            @pl.loop(0, strips)
            def _(part):
                landed(down_got.at[piece, span(part, strip)], downg_recv.at[piece, part])

                @pl.loop(0, strip // down_tile)
                def _(line):
                    index = part * (strip // down_tile) + line
                    some = span(index, down_tile)
                    window = span(piece * (unit_block // down_tile) + index, down_tile)
                    adam(
                        down,
                        down_first,
                        down_second,
                        down_got,
                        down_mine,
                        (window,),
                        (piece, some),
                    )

                pass_down(piece, part).start()

    def average(step):
        for which in range(2):
            index = which * steps + step
            columns = span(block_of(which, step), unit_block)
            landed(up_other.at[index], upl_recv.at[which, step])
            up[:, columns] = 0.5 * (up[:, columns] + up_other[index].astype(F32))

        @pl.when(lax.rem(step, half) == z_slot)
        def _():
            piece = lax.div(step, half)

            @pl.loop(0, strips)
            def _(part):
                some = span(part, strip)
                landed(down_other.at[piece, some], downl_recv.at[piece, part])
                window = span(piece * strips + part, strip)
                down[window, :] = 0.5 * (down[window, :] + down_other[piece, some].astype(F32))

    for copy in states:
        copy.wait()
    delay = jnp.where(worker, jnp.where(first, 1, steps), 0)
    later = jnp.where(worker, steps + 1, 1)

    @pl.loop(0, 2 * steps + 1)
    def _(turn):
        @pl.when(worker & (turn < steps))
        def _():
            compute(turn)

        @pl.when((turn >= delay) & (turn < delay + steps))
        def _():
            update(turn - delay)

        @pl.when((turn >= later) & (turn < later + steps))
        def _():
            average(turn - later)

    for piece in range(chunks):
        for which in range(2):
            give(which, piece).wait_send()

    @pl.when(first)
    def _():
        @pl.loop(0, chunks)
        def _(piece):
            for which in range(2):

                @pl.loop(0, n)
                def _(owner):
                    @pl.when(owner != z)
                    def _():
                        forward(which, owner, piece).wait_send()

    @pl.loop(0, steps)
    def _(step):
        for which in range(2):
            finish_send(give_up(which, step))
            pass_up(which, step).wait_send()

        @pl.when(z_slot == lax.rem(step, half))
        def _():
            finish_send(give_down(lax.div(step, half)))

            @pl.loop(0, strips)
            def _(part):
                pass_down(lax.div(step, half), part).wait_send()

        @pl.when(worker)
        def _():
            for owner in range(n):
                finish_send(give_grads(step, owner))

            @pl.loop(0, strips)
            def _(part):
                finish_send(give_down_grads(step, part))


def fused_step(dist, name, fixes, tokens, out_grad, params):
    n = lax.axis_size("zero")
    own_tokens, width = tokens.shape
    owned = params[1].shape[0]
    units = owned * n
    rows = width // n
    block = min(owned, 256)
    steps = (owned // block) * (n // 2)
    pieces = owned // block
    chunk = min(own_tokens, 128)
    chunks = own_tokens // chunk
    total = n * own_tokens
    strip = min(block, STRIP)
    strips = block // strip
    dims = (n, own_tokens, width, units, block, chunk, strip)
    hbm = pl.BlockSpec(memory_space=pltpu.HBM)
    vmem = pl.BlockSpec(memory_space=pltpu.VMEM)
    dma = pltpu.SemaphoreType.DMA
    up_shape = pltpu.VMEM((rows, units), F32)
    down_shape = pltpu.VMEM((owned, width), F32)
    return pl.pallas_call(
        partial(step_kernel, dist, dims),
        out_shape=(up_shape, down_shape) * 3,
        in_specs=[pl.BlockSpec(memory_space=pltpu.SMEM)] + [hbm] * 8,
        out_specs=(vmem,) * 6,
        scratch_shapes=[
            pltpu.VMEM((total, width), BF16),
            pltpu.VMEM((total, width), BF16),
            pltpu.VMEM((total, width), BF16),
            pltpu.VMEM((width, total), BF16),
            pltpu.VMEM((2 * steps, rows, block), BF16),
            pltpu.VMEM((pieces, block, width), BF16),
            pltpu.VMEM((steps, width, block), BF16),
            pltpu.VMEM((steps, block, width), BF16),
            pltpu.VMEM((block, total), BF16),
            pltpu.VMEM((total, block), BF16),
            pltpu.VMEM((steps, width, block), BF16),
            pltpu.VMEM((steps, block, width), BF16),
            pltpu.VMEM((2 * steps, rows, block), BF16),
            pltpu.VMEM((pieces, block, width), BF16),
            pltpu.VMEM((2 * steps, rows, block), BF16),
            pltpu.VMEM((pieces, block, width), BF16),
            pltpu.VMEM((2 * steps, rows, block), BF16),
            pltpu.VMEM((pieces, block, width), BF16),
            dma((6,)),
            dma((2, chunks)),
            dma((2, n, chunks)),
            dma((2, n, chunks)),
            dma((2, steps)),
            dma((steps, n)),
            dma((pieces,)),
            dma((steps,)),
            dma((steps, n)),
            dma((2, steps)),
            dma((steps, strips)),
            dma((pieces, strips)),
            dma((2, steps)),
            dma((2, steps)),
            dma((pieces, strips)),
            dma((pieces, strips)),
        ],
        compiler_params=pltpu.CompilerParams(
            collective_id=name, has_side_effects=True, vmem_limit_bytes=46 * MIB
        ),
    )(fixes, tokens, out_grad, *params)


def store_kernel(*refs):
    count = len(refs) // 2
    sems = refs[-1]
    copies = [
        pltpu.make_async_copy(refs[index], refs[count + index], sems.at[index])
        for index in range(count)
    ]
    for copy in copies:
        copy.start()
    for copy in copies:
        copy.wait()


def store(arrays):
    return pl.pallas_call(
        store_kernel,
        out_shape=tuple(jax.ShapeDtypeStruct(array.shape, array.dtype) for array in arrays),
        in_specs=[pl.BlockSpec(memory_space=pl.ANY)] * len(arrays),
        out_specs=(pl.BlockSpec(memory_space=pltpu.HBM),) * len(arrays),
        scratch_shapes=[pltpu.SemaphoreType.DMA((len(arrays),))],
        cost_estimate=pl.CostEstimate(flops=10**8, bytes_accessed=24 * MIB, transcendentals=0),
        compiler_params=pltpu.CompilerParams(vmem_limit_bytes=1 * MIB),
    )(*arrays)


def body(
    tokens, out_grad, step, up_param, down_param, up_first, down_first, up_second, down_second
):
    count = (step[0] + 1).astype(F32)
    first_fix = 1.0 - jnp.power(F32(0.9), count)
    second_fix = 1.0 - jnp.power(F32(0.999), count)
    fixes = jnp.stack([0.01 / first_fix, 1.0 / second_fix])
    params = (up_param, down_param, up_first, down_first, up_second, down_second)
    operands = (fixes, tokens[0], out_grad[0], tuple(array[0] for array in params))
    levels = lax.axis_size("peer").bit_length() - 1
    branches = [
        lambda args, level=level: store(fused_step(2**level, level, *args))
        for level in range(levels)
    ]
    results = lax.switch(step[0] % levels, branches, operands)
    return tuple(array[None] for array in results)


def solution(mesh):
    spec = P("peer", "zero", None)
    return jax.shard_map(
        body,
        mesh=mesh,
        in_specs=(spec, spec, P()) + (spec,) * 6,
        out_specs=(spec,) * 6,
        check_vma=False,
    )
```

```python
from functools import partial

import jax
import jax.numpy as jnp
from jax import lax
from jax.experimental import pallas as pl
from jax.experimental.pallas import tpu as pltpu
from jax.sharding import PartitionSpec as P

MIB = 2**20
BF16, F32 = jnp.bfloat16, jnp.float32
EARLY = 1
CHUNK = 256


def step_kernel(
    dist,
    dims,
    fixes,
    tok_in,
    out_in,
    up_in,
    down_in,
    up_first_in,
    down_first_in,
    up_second_in,
    down_second_in,
    up,
    down,
    up_first,
    down_first,
    up_second,
    down_second,
    head,
    held,
    normed,
    normed_t,
    up_stage,
    down_stage,
    up_cols,
    down_rows,
    act_t,
    pre_grad,
    up_grad,
    down_grad,
    up_got,
    down_got,
    up_mine,
    down_mine,
    up_other,
    down_other,
    load_sem,
    tok_send,
    tok_recv,
    fwd_send,
    upw_send,
    upw_recv,
    downw_send,
    downw_recv,
    upg_send,
    upg_recv,
    downg_send,
    downg_recv,
    upl_send,
    upl_recv,
    downl_send,
    downl_recv,
):
    n, tokens, width, units, unit_block, chunk, coarse, fine = dims
    half = n // 2
    rows = width // n
    owned = units // n
    per_owner = owned // unit_block
    steps = per_owner * half
    chunks = tokens // chunk
    total = n * tokens

    z, p = lax.axis_index("zero"), lax.axis_index("peer")
    peers = lax.axis_size("peer")
    side = lax.rem(p, 2)
    base = p - side
    center = half - 1 + side
    worker = (z == half - 1) | (z == half)
    first = worker & (z == center)
    group = base + z - (half - 1)
    z_slot = lax.rem(z, half)
    z_half = lax.div(z, half)

    def at(peer, zero):
        return {"peer": peer, "zero": zero}

    def remote(src, dst, send, recv, peer, zero):
        return pltpu.make_async_remote_copy(
            src_ref=src,
            dst_ref=dst,
            send_sem=send,
            recv_sem=recv,
            device_id=at(peer, zero),
            device_id_type=pl.DeviceIdType.MESH,
        )

    def landed(dst, sem):
        pltpu.make_async_copy(dst, dst, sem).wait()

    def block_of(which, step):
        return which * steps + lax.rem(step, half) * per_owner + lax.div(step, half)

    def span(start, size):
        return pl.ds(pl.multiple_of(start * size, size), size)

    barrier = pltpu.get_barrier_semaphore()

    def greet(peer, zero):
        pl.semaphore_signal(
            barrier, inc=1, device_id=at(peer, zero), device_id_type=pl.DeviceIdType.MESH
        )

    ahead, behind = lax.rem(p + dist, peers), lax.rem(p + peers - dist, peers)
    for other in range(2):

        @pl.when((z != center) | (side != other))
        def _():
            greet(base + other, center)

    for owner in range(n):

        @pl.when(worker & ((group != p) | (z != owner)))
        def _():
            greet(group, owner)

    greet(ahead, z)
    greet(behind, z)

    heads = [
        pltpu.make_async_copy(src.at[pl.ds(0, chunk)], head.at[which], load_sem.at[6 + which])
        for which, src in enumerate((tok_in, out_in))
    ]
    for copy in heads:
        copy.start()
    params = [pltpu.make_async_copy(up_in, up, load_sem.at[0])]
    params.append(pltpu.make_async_copy(down_in, down, load_sem.at[1]))
    states = [
        pltpu.make_async_copy(src, dst, load_sem.at[2 + index])
        for index, (src, dst) in enumerate(
            (
                (up_first_in, up_first),
                (down_first_in, down_first),
                (up_second_in, up_second),
                (down_second_in, down_second),
            )
        )
    ]
    for copy in params:
        copy.start()
    for copy in heads:
        copy.wait()

    once = jnp.where(first, 1, 0)
    pl.semaphore_wait(barrier, 4 - once + jnp.where(worker, n - once, 0))

    sources = (tok_in, out_in)

    def place(owner, piece):
        return span(owner * chunks + piece, chunk)

    def give(which, piece):
        return remote(
            sources[which].at[span(piece, chunk)] if piece else head.at[which],
            held.at[which, place(z, piece)],
            tok_send.at[0],
            tok_recv.at[z, piece],
            jnp.where(z == center, base + 1 - side, p),
            center,
        )

    def keep(which, piece):
        return pltpu.make_async_copy(
            sources[which].at[span(piece, chunk)],
            held.at[which, place(z, piece)],
            tok_recv.at[z, piece],
        )

    def forward(owner, piece):
        spot = held.at[:, place(owner, piece)]
        return remote(
            spot, spot, fwd_send.at[0], tok_recv.at[owner, piece], base + 1 - side, z
        )

    for piece in range(chunks):
        for which in range(2):
            give(which, piece).start()

            @pl.when(first)
            def _():
                keep(which, piece).start()

    for copy in params:
        copy.wait()
    for copy in states:
        copy.start()

    def give_up(which, step):
        index = which * steps + step
        src, dst = up_stage.at[index], up_cols.at[step, span(z, rows)]
        own = partial(pltpu.make_async_copy, src, dst, upw_recv.at[step])
        sent = partial(
            remote, src, dst, upw_send.at[which], upw_recv.at[step], base + which, center
        )
        return own, sent, (z == center) & (side == which)

    def give_down(piece):
        step = piece * half + z_slot
        src, dst = down_stage.at[piece], down_rows.at[step]
        own = partial(pltpu.make_async_copy, src, dst, downw_recv.at[step])
        sent = partial(
            remote, src, dst, downw_send.at[0], downw_recv.at[step], base + z_half, center
        )
        return own, sent, (z == center) & (side == z_half)

    def begin(copies):
        own, sent, mine = copies

        @pl.when(mine)
        def _():
            own().start()

        @pl.when(jnp.logical_not(mine))
        def _():
            sent().start()

    def finish_send(copies):
        _, sent, mine = copies

        @pl.when(jnp.logical_not(mine))
        def _():
            sent().wait_send()

    for step in range(steps):
        for which in range(2):
            block = which * steps + (step % half) * per_owner + step // half
            up_stage[which * steps + step] = up[
                :, block * unit_block : (block + 1) * unit_block
            ].astype(BF16)
            begin(give_up(which, step))
        if step % half == 0:
            piece = step // half
            down_stage[piece] = down[piece * unit_block : (piece + 1) * unit_block].astype(BF16)

        @pl.when(z_slot == step % half)
        def _():
            begin(give_down(step // half))

    @pl.when(worker)
    def _():
        @pl.loop(0, chunks)
        def _(piece):
            @pl.loop(0, n)
            def _(owner):
                spot = place(owner, piece)
                landed(held.at[:, spot], tok_recv.at[owner, piece])

                @pl.when(first & (owner != z))
                def _():
                    forward(owner, piece).start()

                wide = held[0, spot, :].astype(F32)
                mean = jnp.mean(wide, axis=1, keepdims=True)
                wide = wide - mean
                spread = jnp.mean(wide * wide, axis=1, keepdims=True)
                wide = wide * lax.rsqrt(spread + 1e-05)
                normed[spot, :] = wide.astype(BF16)
                normed_t[:, spot] = wide.T.astype(BF16)

    tile = min(total, 256)

    def give_grads(step, owner):
        src, dst = up_grad.at[step, span(owner, rows)], up_got.at[step, side]
        own = partial(pltpu.make_async_copy, src, dst, upg_recv.at[side, step])
        sent = partial(remote, src, dst, upg_send.at[owner], upg_recv.at[side, step], group, owner)
        return own, sent, first & (owner == z)

    def each_strip(step, act):
        piece = lax.div(step, half)

        @pl.when(step < steps - 1)
        def _():
            start = 0
            for index, size in enumerate(coarse):
                act(piece, piece * len(coarse) + index, start, size)
                start += size

        @pl.when(step == steps - 1)
        def _():
            start = 0
            for index, size in enumerate(fine):
                act(piece, (per_owner - 1) * len(coarse) + index, start, size)
                start += size

    def give_down_grads(step, piece, index, start, size):
        slot = lax.rem(step, half)
        owner = side * half + slot
        some = pl.ds(start, size)
        src, dst = down_grad.at[step, some], down_got.at[piece, some]
        own = partial(pltpu.make_async_copy, src, dst, downg_recv.at[index])
        sent = partial(
            remote, src, dst, downg_send.at[slot], downg_recv.at[index], group, owner
        )
        return own, sent, first & (owner == z)

    def spread_grads(step, far):
        for slot in range(half):
            owner = jnp.where((z_half == 0) != far, slot, half + slot)
            begin(give_grads(step, owner))

        @pl.when((side == z_half) != far)
        def _():
            each_strip(step, lambda *strip: begin(give_down_grads(step, *strip)))

    def compute(step):
        landed(up_cols.at[step], upw_recv.at[step])
        landed(down_rows.at[step], downw_recv.at[step])

        @pl.when(step == steps - 1)
        def _():
            @pl.loop(EARLY, steps - 1)
            def _(late):
                spread_grads(late, True)

        @pl.loop(0, total // tile)
        def _(index):
            part = span(index, tile)
            pre = jnp.dot(normed[part, :], up_cols[step], preferred_element_type=F32)
            act_grad = lax.dot_general(
                held[1, part, :], down_rows[step], (((1,), (1,)), ((), ())), preferred_element_type=F32
            )
            square = pre * pre
            bend = jnp.tanh(pre * (0.7978845608 + (0.7978845608 * 0.044715) * square))
            lift = 0.5 + 0.5 * bend
            slope = lift + (0.5 * pre) * (1.0 - bend * bend) * (
                0.7978845608 + (3.0 * 0.7978845608 * 0.044715) * square
            )
            act_t[:, part] = (pre * lift).T.astype(BF16)
            pre_grad[part, :] = (act_grad * slope).astype(BF16)

        @pl.loop(0, width // unit_block)
        def _(index):
            part = span(index, unit_block)
            down_grad[step, :, part] = jnp.dot(
                act_t[...], held[1, :, part], preferred_element_type=F32
            ).astype(BF16)
            up_grad[step, part, :] = jnp.dot(
                normed_t[part, :], pre_grad[...], preferred_element_type=F32
            ).astype(BF16)

        spread_grads(step, False)

        @pl.when((step < EARLY) | (step == steps - 1))
        def _():
            spread_grads(step, True)

    first_scale, second_scale = fixes[0], fixes[1]

    def adam(param, first_ref, second_ref, got, mine, window, piece_window):
        grad = got[piece_window].astype(F32)
        first_new = 0.9 * first_ref[window] + 0.1 * grad
        second_new = 0.999 * second_ref[window] + 0.001 * grad * grad
        first_ref[window] = first_new
        second_ref[window] = second_new
        local = param[window] - (first_new * first_scale) / (
            jnp.sqrt(second_new * second_scale) + 1e-08
        )
        param[window] = local
        mine[piece_window] = local.astype(BF16)

    up_tile, down_tile = min(rows, 32), 16

    def pass_up(which, step):
        return remote(
            up_mine.at[step, which],
            up_other.at[step, which],
            upl_send.at[0],
            upl_recv.at[step],
            behind,
            z,
        )

    def pass_down(piece, index, start, size):
        some = pl.ds(start, size)
        return remote(
            down_mine.at[piece, some],
            down_other.at[piece, some],
            downl_send.at[0],
            downl_recv.at[index],
            behind,
            z,
        )

    def update_strip(piece, index, start, size):
        landed(down_got.at[piece, pl.ds(start, size)], downg_recv.at[index])

        @pl.loop(0, size // down_tile)
        def _(line):
            place_in = start // down_tile + line
            some = span(place_in, down_tile)
            window = span(piece * (unit_block // down_tile) + place_in, down_tile)
            adam(down, down_first, down_second, down_got, down_mine, (window,), (piece, some))

        pass_down(piece, index, start, size).start()

    def average_strip(piece, index, start, size):
        some = pl.ds(start, size)
        landed(down_other.at[piece, some], downl_recv.at[index])
        window = pl.ds(pl.multiple_of(piece * unit_block + start, down_tile), size)
        down[window, :] = 0.5 * (down[window, :] + down_other[piece, some].astype(F32))

    def update_up(which, step):
        landed(up_got.at[step, which], upg_recv.at[which, step])
        columns = span(block_of(which, step), unit_block)

        @pl.loop(0, rows // up_tile)
        def _(part):
            some = span(part, up_tile)
            adam(up, up_first, up_second, up_got, up_mine, (some, columns), (step, which, some))

        pass_up(which, step).start()

    def update(step):
        @pl.when(step == 0)
        def _():
            update_up(side, step)

        update_up(1 - side, step)

        @pl.when(lax.rem(step, half) == z_slot)
        def _():
            each_strip(step, update_strip)

        @pl.when(step < steps - 1)
        def _():
            update_up(side, step + 1)

    def average(step):
        landed(up_other.at[step], upl_recv.at[step])
        for which in range(2):
            columns = span(block_of(which, step), unit_block)
            up[:, columns] = 0.5 * (up[:, columns] + up_other[step, which].astype(F32))

        @pl.when(lax.rem(step, half) == z_slot)
        def _():
            each_strip(step, average_strip)

    def settle():
        landed(held.at[:, pl.ds(0, tokens)], tok_send.at[0])

        @pl.when(first)
        def _():
            landed(held.at[:, pl.ds(0, (n - 1) * tokens)], fwd_send.at[0])

        for which in range(2):

            @pl.when((z != center) | (side != which))
            def _():
                landed(up_stage.at[pl.ds(which * steps, steps)], upw_send.at[which])

        @pl.when((z != center) | (side != z_half))
        def _():
            landed(down_stage, downw_send.at[0])

    for copy in states:
        copy.wait()
    delay = jnp.where(worker, jnp.where(first, 1, steps), 0)
    later = jnp.where(worker, steps + 1, 1)

    @pl.loop(0, 2 * steps + 1)
    def _(turn):
        @pl.when(worker & (turn < steps))
        def _():
            compute(turn)

        @pl.when(turn == delay + steps - 2)
        def _():
            settle()

        @pl.when((turn >= delay) & (turn < delay + steps))
        def _():
            update(turn - delay)

        @pl.when((turn >= later) & (turn < later + steps))
        def _():
            average(turn - later)

    landed(up_mine, upl_send.at[0])
    landed(down_mine, downl_send.at[0])

    @pl.when(worker)
    def _():
        for owner in range(n):

            @pl.when(jnp.logical_not(first & (z == owner)))
            def _():
                landed(up_grad.at[:, pl.ds(owner * rows, rows)], upg_send.at[owner])

        for slot in range(half):

            @pl.when(jnp.logical_not(first & (z == side * half + slot)))
            def _():
                landed(down_grad.at[pl.ds(slot * per_owner, per_owner)], downg_send.at[slot])


def fused_step(dist, name, fixes, tokens, out_grad, params):
    n = lax.axis_size("zero")
    own_tokens, width = tokens.shape
    owned = params[1].shape[0]
    units = owned * n
    rows = width // n
    block = min(owned, 256)
    steps = (owned // block) * (n // 2)
    pieces = owned // block
    chunk = min(own_tokens, CHUNK)
    chunks = own_tokens // chunk
    total = n * own_tokens
    quarter = block // 4
    coarse, fine = (block // 4,) * 4, (quarter,) * 3 + (quarter // 2,) + (quarter // 4,) * 2
    strips = (pieces - 1) * len(coarse) + len(fine)
    dims = (n, own_tokens, width, units, block, chunk, coarse, fine)
    hbm = pl.BlockSpec(memory_space=pltpu.HBM)
    vmem = pl.BlockSpec(memory_space=pltpu.VMEM)
    dma = pltpu.SemaphoreType.DMA
    up_shape = pltpu.VMEM((rows, units), F32)
    down_shape = pltpu.VMEM((owned, width), F32)
    return pl.pallas_call(
        partial(step_kernel, dist, dims),
        out_shape=(up_shape, down_shape) * 3,
        in_specs=[pl.BlockSpec(memory_space=pltpu.SMEM)] + [hbm] * 8,
        out_specs=(vmem,) * 6,
        scratch_shapes=[
            pltpu.VMEM((2, chunk, width), BF16),
            pltpu.VMEM((2, total, width), BF16),
            pltpu.VMEM((total, width), BF16),
            pltpu.VMEM((width, total), BF16),
            pltpu.VMEM((2 * steps, rows, block), BF16),
            pltpu.VMEM((pieces, block, width), BF16),
            pltpu.VMEM((steps, width, block), BF16),
            pltpu.VMEM((steps, block, width), BF16),
            pltpu.VMEM((block, total), BF16),
            pltpu.VMEM((total, block), BF16),
            pltpu.VMEM((steps, width, block), BF16),
            pltpu.VMEM((steps, block, width), BF16),
            pltpu.VMEM((steps, 2, rows, block), BF16),
            pltpu.VMEM((pieces, block, width), BF16),
            pltpu.VMEM((steps, 2, rows, block), BF16),
            pltpu.VMEM((pieces, block, width), BF16),
            pltpu.VMEM((steps, 2, rows, block), BF16),
            pltpu.VMEM((pieces, block, width), BF16),
            dma((8,)),
            dma((1,)),
            dma((n, chunks)),
            dma((1,)),
            dma((2,)),
            dma((steps,)),
            dma((1,)),
            dma((steps,)),
            dma((n,)),
            dma((2, steps)),
            dma((n // 2,)),
            dma((strips,)),
            dma((1,)),
            dma((steps,)),
            dma((1,)),
            dma((strips,)),
        ],
        compiler_params=pltpu.CompilerParams(
            collective_id=name, has_side_effects=True, vmem_limit_bytes=46 * MIB
        ),
    )(fixes, tokens, out_grad, *params)


def store_kernel(*refs):
    count = len(refs) // 2
    sems = refs[-1]
    copies = [
        pltpu.make_async_copy(refs[index], refs[count + index], sems.at[index])
        for index in range(count)
    ]
    for copy in copies:
        copy.start()
    for copy in copies:
        copy.wait()


def store(arrays):
    return pl.pallas_call(
        store_kernel,
        out_shape=tuple(jax.ShapeDtypeStruct(array.shape, array.dtype) for array in arrays),
        in_specs=[pl.BlockSpec(memory_space=pl.ANY)] * len(arrays),
        out_specs=(pl.BlockSpec(memory_space=pltpu.HBM),) * len(arrays),
        scratch_shapes=[pltpu.SemaphoreType.DMA((len(arrays),))],
        cost_estimate=pl.CostEstimate(flops=10**8, bytes_accessed=24 * MIB, transcendentals=0),
        compiler_params=pltpu.CompilerParams(vmem_limit_bytes=1 * MIB),
    )(*arrays)


def body(
    tokens, out_grad, step, up_param, down_param, up_first, down_first, up_second, down_second
):
    count = (step[0] + 1).astype(F32)
    first_fix = 1.0 - jnp.power(F32(0.9), count)
    second_fix = 1.0 - jnp.power(F32(0.999), count)
    fixes = jnp.stack([0.01 / first_fix, 1.0 / second_fix])
    params = (up_param, down_param, up_first, down_first, up_second, down_second)
    operands = (fixes, tokens[0], out_grad[0], tuple(array[0] for array in params))
    levels = lax.axis_size("peer").bit_length() - 1
    branches = [
        lambda args, level=level: store(fused_step(2**level, level, *args))
        for level in range(levels)
    ]
    results = lax.switch(step[0] % levels, branches, operands)
    return tuple(array[None] for array in results)


def solution(mesh):
    spec = P("peer", "zero", None)
    return jax.shard_map(
        body,
        mesh=mesh,
        in_specs=(spec, spec, P()) + (spec,) * 6,
        out_specs=(spec,) * 6,
        check_vma=False,
    )
```

```python
from functools import partial

import jax
import jax.numpy as jnp
from jax import lax
from jax.experimental import pallas as pl
from jax.experimental.pallas import tpu as pltpu
from jax.sharding import PartitionSpec as P

MIB = 2**20
BF16, F32 = jnp.bfloat16, jnp.float32
EARLY = 1
CHUNK = 256


def step_kernel(
    dist,
    dims,
    fixes,
    tok_in,
    out_in,
    up_in,
    down_in,
    up_first_in,
    down_first_in,
    up_second_in,
    down_second_in,
    up,
    down,
    up_first,
    down_first,
    up_second,
    down_second,
    head,
    held,
    normed,
    normed_t,
    up_stage,
    down_stage,
    up_cols,
    down_rows,
    act_t,
    pre_grad,
    up_grad,
    down_grad,
    up_got,
    down_got,
    up_mine,
    down_mine,
    up_other,
    down_other,
    load_sem,
    tok_send,
    tok_recv,
    fwd_send,
    upw_send,
    upw_recv,
    downw_send,
    downw_recv,
    upg_send,
    upg_recv,
    downg_send,
    downg_recv,
    upl_send,
    upl_recv,
    downl_send,
    downl_recv,
):
    n, tokens, width, units, unit_block, chunk, coarse, fine = dims
    half = n // 2
    rows = width // n
    owned = units // n
    per_owner = owned // unit_block
    steps = per_owner * half
    chunks = tokens // chunk
    total = n * tokens

    z, p = lax.axis_index("zero"), lax.axis_index("peer")
    peers = lax.axis_size("peer")
    side = lax.rem(p, 2)
    base = p - side
    center = half - 1 + side
    worker = (z == half - 1) | (z == half)
    first = worker & (z == center)
    group = base + z - (half - 1)
    z_slot = lax.rem(z, half)
    z_half = lax.div(z, half)

    def at(peer, zero):
        return {"peer": peer, "zero": zero}

    def remote(src, dst, send, recv, peer, zero):
        return pltpu.make_async_remote_copy(
            src_ref=src,
            dst_ref=dst,
            send_sem=send,
            recv_sem=recv,
            device_id=at(peer, zero),
            device_id_type=pl.DeviceIdType.MESH,
        )

    def landed(dst, sem):
        pltpu.make_async_copy(dst, dst, sem).wait()

    def block_of(which, step):
        return which * steps + lax.rem(step, half) * per_owner + lax.div(step, half)

    def span(start, size):
        return pl.ds(pl.multiple_of(start * size, size), size)

    barrier = pltpu.get_barrier_semaphore()

    def greet(peer, zero):
        pl.semaphore_signal(
            barrier, inc=1, device_id=at(peer, zero), device_id_type=pl.DeviceIdType.MESH
        )

    ahead, behind = lax.rem(p + dist, peers), lax.rem(p + peers - dist, peers)
    for other in range(2):

        @pl.when((z != center) | (side != other))
        def _():
            greet(base + other, center)

    for owner in range(n):

        @pl.when(worker & ((group != p) | (z != owner)))
        def _():
            greet(group, owner)

    greet(ahead, z)
    greet(behind, z)

    heads = [
        pltpu.make_async_copy(src.at[pl.ds(0, chunk)], head.at[which], load_sem.at[6 + which])
        for which, src in enumerate((tok_in, out_in))
    ]
    for copy in heads:
        copy.start()
    params = [pltpu.make_async_copy(up_in, up, load_sem.at[0])]
    params.append(pltpu.make_async_copy(down_in, down, load_sem.at[1]))
    states = [
        pltpu.make_async_copy(src, dst, load_sem.at[2 + index])
        for index, (src, dst) in enumerate(
            (
                (up_first_in, up_first),
                (down_first_in, down_first),
                (up_second_in, up_second),
                (down_second_in, down_second),
            )
        )
    ]
    for copy in params:
        copy.start()
    once = jnp.where(first, 1, 0)
    pl.semaphore_wait(barrier, 4 - once + jnp.where(worker, n - once, 0))

    sources = (tok_in, out_in)

    def place(owner, piece):
        return span(owner * chunks + piece, chunk)

    def give(which, piece):
        return remote(
            sources[which].at[span(piece, chunk)] if piece else head.at[which],
            held.at[which, place(z, piece)],
            tok_send.at[0],
            tok_recv.at[z, piece],
            jnp.where(z == center, base + 1 - side, p),
            center,
        )

    def keep(which, piece):
        return pltpu.make_async_copy(
            sources[which].at[span(piece, chunk)],
            held.at[which, place(z, piece)],
            tok_recv.at[z, piece],
        )

    def forward(owner, piece):
        spot = held.at[:, place(owner, piece)]
        return remote(
            spot, spot, fwd_send.at[0], tok_recv.at[owner, piece], base + 1 - side, z
        )

    for piece in range(chunks):
        for which in range(2):
            if piece == 0:
                heads[which].wait()
            give(which, piece).start()

    @pl.when(first)
    def _():
        for piece in range(chunks):
            for which in range(2):
                keep(which, piece).start()

    for copy in params:
        copy.wait()
    for copy in states:
        copy.start()

    def give_up(which, step):
        index = which * steps + step
        src, dst = up_stage.at[index], up_cols.at[step, span(z, rows)]
        own = partial(pltpu.make_async_copy, src, dst, upw_recv.at[step])
        sent = partial(
            remote, src, dst, upw_send.at[which], upw_recv.at[step], base + which, center
        )
        return own, sent, (z == center) & (side == which)

    def give_down(piece):
        step = piece * half + z_slot
        src, dst = down_stage.at[piece], down_rows.at[step]
        own = partial(pltpu.make_async_copy, src, dst, downw_recv.at[step])
        sent = partial(
            remote, src, dst, downw_send.at[0], downw_recv.at[step], base + z_half, center
        )
        return own, sent, (z == center) & (side == z_half)

    def begin(copies):
        own, sent, mine = copies

        @pl.when(mine)
        def _():
            own().start()

        @pl.when(jnp.logical_not(mine))
        def _():
            sent().start()

    def finish_send(copies):
        _, sent, mine = copies

        @pl.when(jnp.logical_not(mine))
        def _():
            sent().wait_send()

    for step in range(steps):
        for which in range(2):
            block = which * steps + (step % half) * per_owner + step // half
            up_stage[which * steps + step] = up[
                :, block * unit_block : (block + 1) * unit_block
            ].astype(BF16)
            begin(give_up(which, step))
        if step % half == 0:
            piece = step // half
            down_stage[piece] = down[piece * unit_block : (piece + 1) * unit_block].astype(BF16)

        @pl.when(z_slot == step % half)
        def _():
            begin(give_down(step // half))

    @pl.when(worker)
    def _():
        @pl.loop(0, chunks)
        def _(piece):
            @pl.loop(0, n)
            def _(owner):
                spot = place(owner, piece)
                landed(held.at[:, spot], tok_recv.at[owner, piece])

                @pl.when(first & (owner != z))
                def _():
                    forward(owner, piece).start()

                wide = held[0, spot, :].astype(F32)
                mean = jnp.mean(wide, axis=1, keepdims=True)
                wide = wide - mean
                spread = jnp.mean(wide * wide, axis=1, keepdims=True)
                wide = wide * lax.rsqrt(spread + 1e-05)
                normed[spot, :] = wide.astype(BF16)
                normed_t[:, spot] = wide.T.astype(BF16)

    tile = min(total, 256)

    def give_grads(step, owner):
        src, dst = up_grad.at[step, span(owner, rows)], up_got.at[step, side]
        own = partial(pltpu.make_async_copy, src, dst, upg_recv.at[side, step])
        sent = partial(remote, src, dst, upg_send.at[owner], upg_recv.at[side, step], group, owner)
        return own, sent, first & (owner == z)

    def each_strip(step, act):
        piece = lax.div(step, half)

        @pl.when(step < steps - 1)
        def _():
            start = 0
            for index, size in enumerate(coarse):
                act(piece, piece * len(coarse) + index, start, size)
                start += size

        @pl.when(step == steps - 1)
        def _():
            start = 0
            for index, size in enumerate(fine):
                act(piece, (per_owner - 1) * len(coarse) + index, start, size)
                start += size

    def give_down_grads(step, piece, index, start, size):
        slot = lax.rem(step, half)
        owner = side * half + slot
        some = pl.ds(start, size)
        src, dst = down_grad.at[step, some], down_got.at[piece, some]
        own = partial(pltpu.make_async_copy, src, dst, downg_recv.at[index])
        sent = partial(
            remote, src, dst, downg_send.at[slot], downg_recv.at[index], group, owner
        )
        return own, sent, first & (owner == z)

    def spread_grads(step, far):
        for slot in range(half):
            owner = jnp.where((z_half == 0) != far, slot, half + slot)
            begin(give_grads(step, owner))

        @pl.when((side == z_half) != far)
        def _():
            each_strip(step, lambda *strip: begin(give_down_grads(step, *strip)))

    def compute(step):
        landed(up_cols.at[step], upw_recv.at[step])
        landed(down_rows.at[step], downw_recv.at[step])

        @pl.when(step == steps - 1)
        def _():
            @pl.loop(EARLY, steps - 1)
            def _(late):
                spread_grads(late, True)

        @pl.loop(0, total // tile)
        def _(index):
            part = span(index, tile)
            pre = jnp.dot(normed[part, :], up_cols[step], preferred_element_type=F32)
            act_grad = lax.dot_general(
                held[1, part, :], down_rows[step], (((1,), (1,)), ((), ())), preferred_element_type=F32
            )
            square = pre * pre
            bend = jnp.tanh(pre * (0.7978845608 + (0.7978845608 * 0.044715) * square))
            lift = 0.5 + 0.5 * bend
            slope = lift + (0.5 * pre) * (1.0 - bend * bend) * (
                0.7978845608 + (3.0 * 0.7978845608 * 0.044715) * square
            )
            act_t[:, part] = (pre * lift).T.astype(BF16)
            pre_grad[part, :] = (act_grad * slope).astype(BF16)

        @pl.loop(0, width // unit_block)
        def _(index):
            part = span(index, unit_block)
            down_grad[step, :, part] = jnp.dot(
                act_t[...], held[1, :, part], preferred_element_type=F32
            ).astype(BF16)
            up_grad[step, part, :] = jnp.dot(
                normed_t[part, :], pre_grad[...], preferred_element_type=F32
            ).astype(BF16)

        spread_grads(step, False)

        @pl.when((step < EARLY) | (step == steps - 1))
        def _():
            spread_grads(step, True)

    first_scale, second_scale = fixes[0], fixes[1]

    def adam(param, first_ref, second_ref, got, mine, window, piece_window):
        grad = got[piece_window].astype(F32)
        first_new = 0.9 * first_ref[window] + 0.1 * grad
        second_new = 0.999 * second_ref[window] + 0.001 * grad * grad
        first_ref[window] = first_new
        second_ref[window] = second_new
        local = param[window] - (first_new * first_scale) / (
            jnp.sqrt(second_new * second_scale) + 1e-08
        )
        param[window] = local
        mine[piece_window] = local.astype(BF16)

    up_tile, down_tile = min(rows, 32), 16

    def pass_up(which, step):
        return remote(
            up_mine.at[step, which],
            up_other.at[step, which],
            upl_send.at[0],
            upl_recv.at[step],
            behind,
            z,
        )

    def pass_down(piece, index, start, size):
        some = pl.ds(start, size)
        return remote(
            down_mine.at[piece, some],
            down_other.at[piece, some],
            downl_send.at[0],
            downl_recv.at[index],
            behind,
            z,
        )

    def update_strip(piece, index, start, size):
        landed(down_got.at[piece, pl.ds(start, size)], downg_recv.at[index])

        @pl.loop(0, size // down_tile)
        def _(line):
            place_in = start // down_tile + line
            some = span(place_in, down_tile)
            window = span(piece * (unit_block // down_tile) + place_in, down_tile)
            adam(down, down_first, down_second, down_got, down_mine, (window,), (piece, some))

        pass_down(piece, index, start, size).start()

    def average_strip(piece, index, start, size):
        some = pl.ds(start, size)
        landed(down_other.at[piece, some], downl_recv.at[index])
        window = pl.ds(pl.multiple_of(piece * unit_block + start, down_tile), size)
        down[window, :] = 0.5 * (down[window, :] + down_other[piece, some].astype(F32))

    def update_up(which, step):
        landed(up_got.at[step, which], upg_recv.at[which, step])
        columns = span(block_of(which, step), unit_block)

        @pl.loop(0, rows // up_tile)
        def _(part):
            some = span(part, up_tile)
            adam(up, up_first, up_second, up_got, up_mine, (some, columns), (step, which, some))

        pass_up(which, step).start()

    def update(step):
        @pl.when(step == 0)
        def _():
            update_up(side, step)

        update_up(1 - side, step)

        @pl.when(lax.rem(step, half) == z_slot)
        def _():
            each_strip(step, update_strip)

        @pl.when(step < steps - 1)
        def _():
            update_up(side, step + 1)

    def average(step):
        landed(up_other.at[step], upl_recv.at[step])
        for which in range(2):
            columns = span(block_of(which, step), unit_block)
            up[:, columns] = 0.5 * (up[:, columns] + up_other[step, which].astype(F32))

        @pl.when(lax.rem(step, half) == z_slot)
        def _():
            each_strip(step, average_strip)

    def settle():
        landed(held.at[:, pl.ds(0, tokens)], tok_send.at[0])

        @pl.when(first)
        def _():
            landed(held.at[:, pl.ds(0, (n - 1) * tokens)], fwd_send.at[0])

        for which in range(2):

            @pl.when((z != center) | (side != which))
            def _():
                landed(up_stage.at[pl.ds(which * steps, steps)], upw_send.at[which])

        @pl.when((z != center) | (side != z_half))
        def _():
            landed(down_stage, downw_send.at[0])

    for copy in states:
        copy.wait()
    delay = jnp.where(worker, jnp.where(first, 1, steps), 0)
    later = jnp.where(worker, steps + 1, 1)

    @pl.loop(0, 2 * steps + 1)
    def _(turn):
        @pl.when(worker & (turn < steps))
        def _():
            compute(turn)

        @pl.when(turn == delay + steps - 2)
        def _():
            settle()

        @pl.when((turn >= delay) & (turn < delay + steps))
        def _():
            update(turn - delay)

        @pl.when((turn >= later) & (turn < later + steps))
        def _():
            average(turn - later)

    landed(up_mine, upl_send.at[0])
    landed(down_mine, downl_send.at[0])

    @pl.when(worker)
    def _():
        for owner in range(n):

            @pl.when(jnp.logical_not(first & (z == owner)))
            def _():
                landed(up_grad.at[:, pl.ds(owner * rows, rows)], upg_send.at[owner])

        for slot in range(half):

            @pl.when(jnp.logical_not(first & (z == side * half + slot)))
            def _():
                landed(down_grad.at[pl.ds(slot * per_owner, per_owner)], downg_send.at[slot])


def fused_step(dist, name, fixes, tokens, out_grad, params):
    n = lax.axis_size("zero")
    own_tokens, width = tokens.shape
    owned = params[1].shape[0]
    units = owned * n
    rows = width // n
    block = min(owned, 256)
    steps = (owned // block) * (n // 2)
    pieces = owned // block
    chunk = min(own_tokens, CHUNK)
    chunks = own_tokens // chunk
    total = n * own_tokens
    quarter = block // 4
    coarse, fine = (block // 4,) * 4, (quarter,) * 3 + (quarter // 2,) + (quarter // 4,) * 2
    strips = (pieces - 1) * len(coarse) + len(fine)
    dims = (n, own_tokens, width, units, block, chunk, coarse, fine)
    hbm = pl.BlockSpec(memory_space=pltpu.HBM)
    vmem = pl.BlockSpec(memory_space=pltpu.VMEM)
    dma = pltpu.SemaphoreType.DMA
    up_shape = pltpu.VMEM((rows, units), F32)
    down_shape = pltpu.VMEM((owned, width), F32)
    return pl.pallas_call(
        partial(step_kernel, dist, dims),
        out_shape=(up_shape, down_shape) * 3,
        in_specs=[pl.BlockSpec(memory_space=pltpu.SMEM)] + [hbm] * 8,
        out_specs=(vmem,) * 6,
        scratch_shapes=[
            pltpu.VMEM((2, chunk, width), BF16),
            pltpu.VMEM((2, total, width), BF16),
            pltpu.VMEM((total, width), BF16),
            pltpu.VMEM((width, total), BF16),
            pltpu.VMEM((2 * steps, rows, block), BF16),
            pltpu.VMEM((pieces, block, width), BF16),
            pltpu.VMEM((steps, width, block), BF16),
            pltpu.VMEM((steps, block, width), BF16),
            pltpu.VMEM((block, total), BF16),
            pltpu.VMEM((total, block), BF16),
            pltpu.VMEM((steps, width, block), BF16),
            pltpu.VMEM((steps, block, width), BF16),
            pltpu.VMEM((steps, 2, rows, block), BF16),
            pltpu.VMEM((pieces, block, width), BF16),
            pltpu.VMEM((steps, 2, rows, block), BF16),
            pltpu.VMEM((pieces, block, width), BF16),
            pltpu.VMEM((steps, 2, rows, block), BF16),
            pltpu.VMEM((pieces, block, width), BF16),
            dma((8,)),
            dma((1,)),
            dma((n, chunks)),
            dma((1,)),
            dma((2,)),
            dma((steps,)),
            dma((1,)),
            dma((steps,)),
            dma((n,)),
            dma((2, steps)),
            dma((n // 2,)),
            dma((strips,)),
            dma((1,)),
            dma((steps,)),
            dma((1,)),
            dma((strips,)),
        ],
        compiler_params=pltpu.CompilerParams(
            collective_id=name, has_side_effects=True, vmem_limit_bytes=46 * MIB
        ),
    )(fixes, tokens, out_grad, *params)


def store_kernel(*refs):
    count = len(refs) // 2
    sems = refs[-1]
    copies = [
        pltpu.make_async_copy(refs[index], refs[count + index], sems.at[index])
        for index in range(count)
    ]
    for copy in copies:
        copy.start()
    for copy in copies:
        copy.wait()


def store(arrays):
    return pl.pallas_call(
        store_kernel,
        out_shape=tuple(jax.ShapeDtypeStruct(array.shape, array.dtype) for array in arrays),
        in_specs=[pl.BlockSpec(memory_space=pl.ANY)] * len(arrays),
        out_specs=(pl.BlockSpec(memory_space=pltpu.HBM),) * len(arrays),
        scratch_shapes=[pltpu.SemaphoreType.DMA((len(arrays),))],
        cost_estimate=pl.CostEstimate(flops=10**8, bytes_accessed=24 * MIB, transcendentals=0),
        compiler_params=pltpu.CompilerParams(vmem_limit_bytes=1 * MIB),
    )(*arrays)


def body(
    tokens, out_grad, step, up_param, down_param, up_first, down_first, up_second, down_second
):
    count = (step[0] + 1).astype(F32)
    first_fix = 1.0 - jnp.power(F32(0.9), count)
    second_fix = 1.0 - jnp.power(F32(0.999), count)
    fixes = jnp.stack([0.01 / first_fix, 1.0 / second_fix])
    params = (up_param, down_param, up_first, down_first, up_second, down_second)
    operands = (fixes, tokens[0], out_grad[0], tuple(array[0] for array in params))
    levels = lax.axis_size("peer").bit_length() - 1
    branches = [
        lambda args, level=level: store(fused_step(2**level, level, *args))
        for level in range(levels)
    ]
    results = lax.switch(step[0] % levels, branches, operands)
    return tuple(array[None] for array in results)


def solution(mesh):
    spec = P("peer", "zero", None)
    return jax.shard_map(
        body,
        mesh=mesh,
        in_specs=(spec, spec, P()) + (spec,) * 6,
        out_specs=(spec,) * 6,
        check_vma=False,
    )
```
